512 devices in a mesh: occ: 128 (over z_hi, x, y), aux: 4 (over z_lo, core).
Axes of the slice: x: 4, y: 8, z: 8 (z_hi: 4, z_lo: 2; z = z_hi * 2 + z_lo), core: 2. Of those that a mesh axis runs over, the one named last changes fastest.
Arguments:
- factors: bfloat16 [128, 512, 2048], P('occ', None, 'aux'), may hold values from -0.8984375 to 0.8984375
- offsets: int32 [2], replicated, may hold values from 1 to 127, as said below
- occ_energy: float32 [128], replicated, may hold values from -2 to -0.5
- vir_energy: float32 [512], replicated, may hold values from 0.2 to 3
Outputs:
- gamma: float32 [128, 512, 2048], P('occ', None, 'aux')
- vir_density: float32 [512, 512], P('aux')
The draws below stay inside these ranges and needn't reach their ends.
Inputs may be any that keep to these rules, and one draw needn't show every extreme that they name: `offsets`: distinct.
All inputs are finite; a program needn't handle non-finite values.
Results may differ from the reference program's by a relative error of at most 0.0027.
Values may be sent and summed in bfloat16 or wider, within the bound.
No kernel may reach another device: no remote copies, remote signals or barrier semaphores. Data moves between devices by JAX's collectives and lax.ppermute only.
A program may use at most 128 MiB of HBM per device.

```python
import jax
import jax.numpy as jnp
from jax import lax

NV = 512
NAUX = 2048
NOFF = 2
NOCC = 128


def draw_offsets(key, part):
    first_key = jax.random.fold_in(key, 11)
    order_key = jax.random.fold_in(key, 23)
    others = jax.random.permutation(first_key, NOCC - 2)[:NOFF - 1] + 1
    top_value = jnp.full((1,), NOCC - 1, dtype=jnp.int32)
    picked = jnp.concatenate([top_value, others.astype(jnp.int32)])
    placed = jax.random.permutation(order_key, picked)
    return placed.astype(jnp.int32)


def shard_levels(key, shape, cuts, smallest, high):
    def one(axis_at, parts):
        draws = jax.random.uniform(jax.random.fold_in(jax.random.fold_in(key, 6), axis_at), (parts,), jnp.float32, smallest / len(cuts), high / len(cuts))
        return jnp.repeat(jnp.exp(draws), shape[axis_at] // parts).reshape((-1,) + (1,) * (len(shape) - axis_at - 1))

    factor_of = one(*cuts[0])
    for cut in cuts[1:]:
        factor_of = factor_of * one(*cut)
    return factor_of


def normal_values(key, dims, spread, bound, pieces=(), held_as=jnp.bfloat16):
    level = shard_levels(key, dims, pieces, -0.22, 0.18) if pieces else 1.0
    entries = jax.random.normal(key, dims, jnp.float32) * spread * level
    return jnp.minimum(jnp.maximum(entries, -bound), bound).astype(held_as)


def setup_inputs(seed: int = 0) -> dict:
    arg_keys = jax.random.split(jax.random.key(seed), 5)
    factors = normal_values(arg_keys[0], (NOCC, NV, NAUX), 0.15, 0.8984375, ((0, 128), (2, 4)))
    offsets = draw_offsets(jax.random.fold_in(arg_keys[4], 71), 0)
    occ_energy = jnp.clip(jax.random.uniform(arg_keys[2], (NOCC,), jnp.float32, -2.0, -0.5), -2.0, -0.5)
    vir_energy = jnp.clip(jax.random.uniform(arg_keys[3], (NV,), jnp.float32, 0.2, 3.0), 0.2, 3.0)
    return {"factors": factors, "offsets": offsets, "occ_energy": occ_energy, "vir_energy": vir_energy}


def reference(factors, offsets, occ_energy, vir_energy):
    gamma = jnp.zeros((NOCC, NV, NAUX), jnp.float32)
    density = jnp.zeros((NV, NV), jnp.float32)
    hp = lax.Precision.HIGHEST
    for k in range(NOFF):
        shift_by = offsets[k]

        def one(dens, index):
            partner = (index + shift_by) % NOCC
            left = factors[index].astype(jnp.float32)
            right = factors[partner].astype(jnp.float32)
            pair = jnp.dot(left, right.T, precision=hp, preferred_element_type=jnp.float32)
            denom = occ_energy[index] + occ_energy[partner] - vir_energy[:, None] - vir_energy[None, :]
            amp = pair / denom
            mixed = (2.0 * amp - amp.T).astype(jnp.bfloat16).astype(jnp.float32)
            amp_b = amp.astype(jnp.bfloat16).astype(jnp.float32)
            own = jnp.dot(mixed, right, precision=hp, preferred_element_type=jnp.float32)
            back = jnp.dot(mixed.T, left, precision=hp, preferred_element_type=jnp.float32).astype(jnp.bfloat16)
            dens = dens + jnp.dot(amp_b, mixed.T, precision=hp, preferred_element_type=jnp.float32)
            return dens, (own, back)

        density, (own_terms, back_terms) = lax.scan(one, density, jnp.arange(NOCC, dtype=jnp.int32))
        gamma = gamma + own_terms
        gamma = gamma + jnp.roll(back_terms.astype(jnp.float32), shift_by, axis=0)
    return gamma, density
```

```python
import jax
import jax.numpy as jnp
from jax import lax
from jax.sharding import Mesh
from jax.sharding import PartitionSpec as P

OCC = ("zh", "x", "y")
ROWS = ("zh", "x")


def exchange(value, axis):
    return lax.all_to_all(value, axis, split_axis=0, concat_axis=0, tiled=True)


def swap(value, axis):
    return lax.ppermute(value, axis, [(0, 1), (1, 0)])


def to_pieces(block, peers):
    tall, wide = block.shape
    tiles = block.reshape(tall // 8, 8, wide // 128, 128).transpose(0, 2, 1, 3)
    return tiles.reshape(peers, -1, 128)


def from_pieces(pieces, tall, wide):
    tiles = pieces.reshape(tall // 8, wide // 128, 8, 128).transpose(0, 2, 1, 3)
    return tiles.reshape(tall, wide)


def inner(left, right):
    return lax.dot_general(
        left, right, (((1,), (1,)), ((), ())), preferred_element_type=jnp.float32
    )


def local(factors, offsets, occ_energy, vir_energy):
    count = lax.axis_size(OCC)
    myself = lax.axis_index(OCC)
    core = lax.axis_index("core")
    section = lax.axis_index("zl") * 2 + core
    own = factors[0]
    nvir, width = own.shape
    half = nvir // 2
    rows = nvir // 4
    noff = offsets.shape[0]

    held = exchange(to_pieces(own, count), OCC)
    twice = jnp.concatenate([held, held], axis=0)
    depth = held.shape[1]

    def deliver(starts):
        rolled = [lax.dynamic_slice_in_dim(twice, s, count, 0) for s in starts]
        got = exchange(jnp.concatenate(rolled, axis=1), OCC)
        return [
            from_pieces(got[:, k * depth : (k + 1) * depth], nvir, width)
            for k in range(len(starts))
        ]

    ahead = deliver([offsets[k] for k in range(noff)])
    behind = deliver([count - offsets[k] for k in range(noff)])
    e_own = lax.dynamic_index_in_dim(occ_energy, myself, 0, keepdims=False)
    base = e_own - vir_energy[:, None] - vir_energy[None, :]

    def amplitudes(partners, shifts):
        mine = lax.dynamic_slice_in_dim(own, core * half, half, 0)
        other = lax.dynamic_slice_in_dim(own, (1 - core) * half, half, 0)
        kept = jnp.stack([inner(mine, p) for p in partners])
        sent = jnp.stack([inner(other, p) for p in partners])
        chip = kept + swap(sent, "core")
        pair = chip + swap(chip.astype(jnp.bfloat16), "zl").astype(jnp.float32)
        there = swap(pair, "core")
        first = jnp.where(core == 0, pair, there)
        second = jnp.where(core == 0, there, pair)
        whole = jnp.concatenate([first, second], axis=1)
        amps = []
        for k, shift in enumerate(shifts):
            e_partner = lax.dynamic_index_in_dim(
                occ_energy, (myself + shift) % count, 0, keepdims=False
            )
            amps.append(whole[k] / (base + e_partner))
        return amps

    def mix(amp):
        return (2.0 * amp - amp.T).astype(jnp.bfloat16)

    amps = amplitudes(ahead, [offsets[k] for k in range(noff)])
    mixes = [mix(a) for a in amps]
    density = jnp.zeros((rows, nvir), jnp.float32)
    for amp, mixed in zip(amps, mixes):
        part = lax.dynamic_slice_in_dim(amp, section * rows, rows, 0)
        density = density + inner(part.astype(jnp.bfloat16), mixed)

    ny = lax.axis_size("y")
    nrow = lax.axis_size(ROWS)
    sent = density.astype(jnp.bfloat16).reshape(ny, rows // ny, nvir)
    summed = jnp.sum(exchange(sent, "y").astype(jnp.float32), axis=0)
    spread = jnp.broadcast_to(summed.astype(jnp.bfloat16), (nrow, *summed.shape))
    summed = jnp.sum(exchange(spread, ROWS).astype(jnp.float32), axis=0)
    spread = jnp.broadcast_to(summed.astype(jnp.bfloat16), (ny, *summed.shape))
    total = exchange(spread, "y").reshape(rows, nvir).astype(jnp.float32)

    back = amplitudes(behind, [count - offsets[k] for k in range(noff)])
    gamma = jnp.zeros(own.shape, jnp.float32)
    for mixed, block in zip(mixes + [mix(a) for a in back], ahead + behind):
        gamma = gamma + jnp.dot(mixed, block, preferred_element_type=jnp.float32)
    return (gamma[None], total)


def solution(mesh):
    split = Mesh(
        mesh.devices.reshape(4, 4, 8, 2, 2), ("zh", "x", "y", "zl", "core")
    )
    aux = ("zl", "core")
    return jax.shard_map(
        local,
        mesh=split,
        in_specs=(P(OCC, None, aux), P(), P(), P()),
        out_specs=(P(OCC, None, aux), P(aux, None)),
        check_vma=False,
    )
```

```python
import functools

import jax
import jax.numpy as jnp
from jax import lax
from jax.experimental import pallas as pl
from jax.experimental.pallas import tpu as pltpu
from jax.sharding import Mesh
from jax.sharding import PartitionSpec as P

OCC = ("zh", "x", "y")
REST = ("zh", "x", "zl")
SUB = 16
LANES = 128
VMEM = pl.BlockSpec(memory_space=pltpu.VMEM)
SMEM = pl.BlockSpec(memory_space=pltpu.SMEM)
ANY = pl.BlockSpec(memory_space=pl.ANY)
SMALL = pltpu.CompilerParams(vmem_limit_bytes=16 << 20)


def near(value):
    return pltpu.with_memory_space_constraint(value, pltpu.VMEM)


def far(value):
    return pltpu.with_memory_space_constraint(value, pltpu.HBM)


def exchange(value, axis):
    return lax.all_to_all(value, axis, split_axis=0, concat_axis=0, tiled=True)


def swap(value, axis):
    return lax.ppermute(value, axis, [(0, 1), (1, 0)])


def inner(left, right):
    return lax.dot_general(
        left, right, (((1,), (1,)), ((), ())), preferred_element_type=jnp.float32
    )


def to_pieces(block):
    tall, wide = block.shape
    tiles = block.reshape(tall // SUB, SUB, wide // LANES, LANES)
    return tiles.transpose(0, 2, 1, 3).reshape(-1, SUB, LANES)


def roll_kernel(starts_ref, held_ref, out_ref, twice_ref, sems):
    count = held_ref.shape[0]
    twice_ref[:count] = held_ref[...]
    twice_ref[count:] = held_ref[...]
    copies = []
    for k in range(starts_ref.shape[0]):
        copies.append(
            pltpu.make_async_copy(
                twice_ref.at[pl.ds(starts_ref[k], count)],
                out_ref.at[:, pl.ds(k * SUB, SUB), :],
                sems.at[k],
            )
        )
        copies[-1].start()
    for copy in copies:
        copy.wait()


def rolled(starts, held):
    count, sub, lanes = held.shape
    total = starts.shape[0]
    return pl.pallas_call(
        roll_kernel,
        out_shape=pltpu.HBM((count, total * sub, lanes), held.dtype),
        in_specs=[SMEM, VMEM],
        out_specs=ANY,
        compiler_params=SMALL,
        scratch_shapes=[
            pltpu.VMEM((2 * count, sub, lanes), held.dtype),
            pltpu.SemaphoreType.DMA((total,)),
        ],
    )(starts, near(held))


def partial_kernel(
    group, place_ref, own_ref, got_ref, block_ref, kept_ref, sent_ref, held_ref, mine_ref,
    sems,
):
    noff, tall, wide = held_ref.shape
    half = tall // 2
    core = place_ref[1]
    for k in range(noff):
        first = (group * noff + k) * SUB
        for c in range(wide // LANES):
            tile = got_ref[:, c, first : first + SUB, :]
            held_ref[k, :, c * LANES : (c + 1) * LANES] = tile.reshape(tall, LANES)
    copies = [
        pltpu.make_async_copy(held_ref, block_ref, sems.at[0]),
        pltpu.make_async_copy(mine_ref, kept_ref, sems.at[1]),
    ]
    copies[0].start()
    mine = own_ref[pl.ds(pl.multiple_of(core * half, half), half), :]
    other = own_ref[pl.ds(pl.multiple_of((1 - core) * half, half), half), :]
    for k in range(noff):
        mine_ref[k] = inner(mine, held_ref[k])
    copies[1].start()
    for k in range(noff):
        sent_ref[k] = inner(other, held_ref[k])
    for copy in copies:
        copy.wait()


def partials(place, own, got, group):
    tall, wide = own.shape
    noff = got.shape[1] // SUB // 2
    got = got.reshape(tall // SUB, wide // LANES, 2 * noff * SUB, LANES)
    half, whole = (noff, tall // 2, tall), (noff, tall, wide)
    return pl.pallas_call(
        functools.partial(partial_kernel, group),
        out_shape=(
            pltpu.HBM(whole, own.dtype),
            pltpu.HBM(half, jnp.float32),
            jax.ShapeDtypeStruct(half, jnp.float32),
        ),
        in_specs=[SMEM, VMEM, VMEM],
        out_specs=(ANY, ANY, VMEM),
        compiler_params=SMALL,
        scratch_shapes=[
            pltpu.VMEM(whole, own.dtype),
            pltpu.VMEM(half, jnp.float32),
            pltpu.SemaphoreType.DMA((2,)),
        ],
    )(place, own, near(got))


def amplitude(place_ref, shift, occ_ref, row_ref, pair, there, amp_ref):
    me, core = place_ref[0], place_ref[1]
    half, _ = pair.shape
    energy = occ_ref[me] + occ_ref[lax.rem(me + shift, occ_ref.shape[0])]
    row = row_ref[...]
    for value, place in ((pair, core), (there, 1 - core)):
        start = pl.multiple_of(place * half, half)
        mine = row_ref[:, pl.ds(start, half)]
        column = jnp.broadcast_to(mine, (LANES, half)).T[:, :1]
        amp_ref[pl.ds(start, half), :] = value / (energy - column - row)
    return amp_ref[...]


def first_kernel(
    place_ref, shifts_ref, occ_ref, row_ref, pair_ref, there_ref,
    mixed_ref, density_ref, amp_ref, held_ref, sem,
):
    core, chip = place_ref[1], place_ref[2]
    slots, chips, depth, _ = density_ref.shape
    rows = slots * depth
    amp = amplitude(
        place_ref, shifts_ref[chip], occ_ref, row_ref, pair_ref[...], there_ref[...], amp_ref
    )
    held_ref[...] = (2.0 * amp - amp.T).astype(held_ref.dtype)
    out = pltpu.make_async_copy(held_ref, mixed_ref, sem)
    out.start()
    for s in range(chips):
        at = pl.ds(pl.multiple_of((chips * s + core) * rows, rows), rows)
        part = inner(amp_ref[at, :].astype(held_ref.dtype), held_ref[...])
        part = part.astype(density_ref.dtype)
        density_ref[:, s] = part.reshape(slots, depth, part.shape[1])
    out.wait()


def first_pair(place, shifts, occ, row, pair, there, slots):
    _, nvir = pair.shape
    return pl.pallas_call(
        first_kernel,
        out_shape=(
            pltpu.HBM((nvir, nvir), jnp.bfloat16),
            pltpu.HBM((slots, 2, nvir // 4 // slots, nvir), jnp.bfloat16),
        ),
        in_specs=[SMEM, SMEM, SMEM, VMEM, VMEM, VMEM],
        out_specs=(ANY, VMEM),
        compiler_params=SMALL,
        scratch_shapes=[
            pltpu.VMEM((nvir, nvir), jnp.float32),
            pltpu.VMEM((nvir, nvir), jnp.bfloat16),
            pltpu.SemaphoreType.DMA,
        ],
    )(place, shifts, occ, row, near(pair), near(there))


def product_kernel(place_ref, mixed_ref, block_ref, out_ref):
    block = block_ref[place_ref[2]]
    out_ref[...] = jnp.dot(mixed_ref[...], block, preferred_element_type=jnp.float32)


def product(place, mixed, block):
    return pl.pallas_call(
        product_kernel,
        out_shape=pltpu.HBM(block.shape[1:], jnp.float32),
        in_specs=[SMEM, VMEM, VMEM],
        out_specs=VMEM,
        compiler_params=SMALL,
    )(place, far(mixed), far(block))


def rest_kernel(
    place_ref, shifts_ref, occ_ref, row_ref, pair_ref, there_ref, ahead_ref, behind_ref,
    sofar_ref, gamma_ref, amp_ref, block_ref, total_ref, sems,
):
    other = 1 - place_ref[2]
    copies = [
        pltpu.make_async_copy(sofar_ref, total_ref, sems.at[0]),
        pltpu.make_async_copy(ahead_ref.at[other], block_ref.at[0], sems.at[1]),
        pltpu.make_async_copy(behind_ref, block_ref.at[pl.ds(1, 2)], sems.at[2]),
    ]
    for copy in copies:
        copy.start()
    for k in range(pair_ref.shape[0]):
        shift = shifts_ref[other if k == 0 else k + 1]
        amp = amplitude(place_ref, shift, occ_ref, row_ref, pair_ref[k], there_ref[k], amp_ref)
        mixed = (2.0 * amp - amp.T).astype(block_ref.dtype)
        if k == 0:
            copies[0].wait()
            copies[1].wait()
        if k == 1:
            copies[2].wait()
        part = jnp.dot(mixed, block_ref[k], preferred_element_type=jnp.float32)
        gamma_ref[...] = (total_ref[...] if k == 0 else gamma_ref[...]) + part


def add_rest(place, shifts, occ, row, pair, there, ahead, behind, sofar):
    npair = pair.shape[0]
    return pl.pallas_call(
        rest_kernel,
        out_shape=jax.ShapeDtypeStruct(sofar.shape, jnp.float32),
        in_specs=[SMEM, SMEM, SMEM, VMEM, VMEM, VMEM, ANY, ANY, ANY],
        out_specs=VMEM,
        compiler_params=SMALL,
        scratch_shapes=[
            pltpu.VMEM((pair.shape[2],) * 2, jnp.float32),
            pltpu.VMEM((npair, *ahead.shape[1:]), ahead.dtype),
            pltpu.VMEM(sofar.shape, jnp.float32),
            pltpu.SemaphoreType.DMA((3,)),
        ],
    )(place, shifts, occ, row, pair, there, far(ahead), far(behind), far(sofar))


def local(factors, offsets, occ_energy, vir_energy):
    count = lax.axis_size(OCC)
    chip = lax.axis_index("zl").astype(jnp.int32)
    core = lax.axis_index("core").astype(jnp.int32)
    place = jnp.stack([lax.axis_index(OCC).astype(jnp.int32), core, chip])
    own = factors[0]
    nvir = own.shape[0]
    rows = nvir // 4
    row = vir_energy[None, :]
    shifts = jnp.concatenate([offsets, count - offsets])

    held = exchange(to_pieces(own), OCC)
    outgoing = rolled(shifts, held)
    got = exchange(outgoing, OCC)

    ahead, kept, sent = partials(place, own, got, 0)
    came = swap(sent, "core")
    total = kept + came
    mine = lax.dynamic_index_in_dim(total, chip, 0, keepdims=False)
    yours = lax.dynamic_index_in_dim(total, 1 - chip, 0, keepdims=False)
    sent = yours.astype(jnp.bfloat16)
    came = swap(sent, "zl")
    pair = mine + came.astype(jnp.float32)
    there = swap(pair, "core")
    mixed, density = first_pair(
        place, shifts, occ_energy, row, pair, there, lax.axis_size("y")
    )

    behind, kept, sent = partials(place, own, got, 1)
    came = swap(sent, "core")
    back = kept + came
    sent = jnp.concatenate([mine[None], back]).astype(jnp.bfloat16)
    came = swap(sent, "zl")
    pair = jnp.concatenate([yours[None], back]) + came.astype(jnp.float32)
    there = swap(pair, "core")
    sofar = product(place, mixed, ahead)
    gamma = add_rest(place, shifts, occ_energy, row, pair, there, ahead, behind, sofar)

    ny = lax.axis_size("y")
    nrest = lax.axis_size(REST) // 2
    came = exchange(density, "y")
    summed = jnp.sum(came.astype(jnp.float32), axis=0).astype(jnp.bfloat16)
    sent = jnp.broadcast_to(summed, (nrest, *summed.shape)).reshape(
        2 * nrest, rows // ny, nvir
    )
    came = exchange(sent, REST)
    summed = jnp.sum(came.astype(jnp.float32), axis=0).astype(jnp.bfloat16)
    sent = jnp.broadcast_to(summed, (ny, *summed.shape))
    came = exchange(sent, "y")
    return (gamma[None], came.reshape(rows, nvir).astype(jnp.float32))


def solution(mesh):
    split = Mesh(
        mesh.devices.reshape(4, 4, 8, 2, 2), ("zh", "x", "y", "zl", "core")
    )
    aux = ("zl", "core")

    return jax.shard_map(
        local,
        mesh=split,
        in_specs=(P(OCC, None, aux), P(), P(), P()),
        out_specs=(P(OCC, None, aux), P(aux, None)),
        check_vma=False,
    )
```

```python
import jax
import jax.numpy as jnp
from jax import lax
from jax.experimental import pallas as pl
from jax.experimental.pallas import tpu as pltpu
from jax.sharding import Mesh
from jax.sharding import PartitionSpec as P

OCC = ("zh", "x", "y")
ROWS = ("zh", "x")
ROW = 8
SUB = 16
LANES = 128
VMEM = pl.BlockSpec(memory_space=pltpu.VMEM)
SMEM = pl.BlockSpec(memory_space=pltpu.SMEM)
ANY = pl.BlockSpec(memory_space=pl.ANY)
SMALL = pltpu.CompilerParams(vmem_limit_bytes=16 << 20)


def near(value):
    return pltpu.with_memory_space_constraint(value, pltpu.VMEM)


def far(value):
    return pltpu.with_memory_space_constraint(value, pltpu.HBM)


def exchange(value, axis):
    return lax.all_to_all(value, axis, split_axis=0, concat_axis=0, tiled=True)


def swap(value, axis):
    return lax.ppermute(value, axis, [(0, 1), (1, 0)])


def inner(left, right):
    return lax.dot_general(
        left, right, (((1,), (1,)), ((), ())), preferred_element_type=jnp.float32
    )


def busiest_link(shift, sizes):
    count = sizes[0] * sizes[1] * sizes[2]
    load = {}

    def split(i):
        return [i // (sizes[1] * sizes[2]), i // sizes[2] % sizes[1], i % sizes[2]]

    for i in range(count):
        at, goal = split((i + shift) % count), split(i)
        for d, hops in ((1, 1), (2, 1), (0, 2)):
            gap = (goal[d] - at[d]) % sizes[d]
            ways = [(1, gap)] if 2 * gap < sizes[d] else [(-1, sizes[d] - gap)]
            if 2 * gap == sizes[d]:
                ways = [(1, gap), (-1, gap)]
            for sign, steps in ways:
                spot = list(at)
                for _ in range(steps):
                    link = (d, sign, tuple(spot))
                    load[link] = load.get(link, 0) + (2 * hops if d == 0 else 2) // len(ways)
                    spot[d] = (spot[d] + sign) % sizes[d]
            at[d] = goal[d]
    return max(load.values())


def fetch_both_ways(block, amount, count):
    def branch(step):
        ahead = [(i, (i - step) % count) for i in range(count)]
        behind = [(i, (i + step) % count) for i in range(count)]
        return lambda v: (lax.ppermute(v, OCC, ahead), lax.ppermute(v, OCC, behind))

    return lax.switch(amount - 1, [branch(s) for s in range(1, count // 2 + 1)], block)


def to_pieces(block):
    tall, wide = block.shape
    tiles = block.reshape(tall // ROW, ROW, wide // LANES, LANES)
    return tiles.transpose(0, 2, 1, 3).reshape(-1, SUB, LANES)


def roll_kernel(starts_ref, held_ref, out_ref, twice_ref, sems):
    count = held_ref.shape[0]
    twice_ref[:count] = held_ref[...]
    twice_ref[count:] = held_ref[...]
    copies = []
    for k in range(starts_ref.shape[0]):
        copies.append(
            pltpu.make_async_copy(
                twice_ref.at[pl.ds(starts_ref[k], count)],
                out_ref.at[:, pl.ds(k * SUB, SUB), :],
                sems.at[k],
            )
        )
        copies[-1].start()
    for copy in copies:
        copy.wait()


def rolled(starts, held):
    count, sub, lanes = held.shape
    total = starts.shape[0]
    return pl.pallas_call(
        roll_kernel,
        out_shape=pltpu.HBM((count, total * sub, lanes), held.dtype),
        in_specs=[SMEM, VMEM],
        out_specs=ANY,
        compiler_params=SMALL,
        scratch_shapes=[
            pltpu.VMEM((2 * count, sub, lanes), held.dtype),
            pltpu.SemaphoreType.DMA((total,)),
        ],
    )(starts, near(held))


def pair_products(place_ref, own_ref, block_of, mine_ref, kept_ref, sent_ref, sem):
    noff, half, _ = mine_ref.shape
    core = place_ref[1]
    mine = own_ref[pl.ds(pl.multiple_of(core * half, half), half), :]
    other = own_ref[pl.ds(pl.multiple_of((1 - core) * half, half), half), :]
    for k in range(noff):
        mine_ref[k] = inner(mine, block_of(k))
    out = pltpu.make_async_copy(mine_ref, kept_ref, sem)
    out.start()
    for k in range(noff):
        sent_ref[k] = inner(other, block_of(k))
    return out


def direct_kernel(
    place_ref, own_ref, ahead_ref, behind_ref, kept_ref, sent_ref, mine_ref, sem
):
    refs = (ahead_ref, behind_ref)
    pair_products(
        place_ref, own_ref, lambda k: refs[k][...], mine_ref, kept_ref, sent_ref, sem
    ).wait()


def partials_direct(place, own, ahead, behind):
    tall, _ = own.shape
    half = (2, tall // 2, tall)
    return pl.pallas_call(
        direct_kernel,
        out_shape=(pltpu.HBM(half, jnp.float32), jax.ShapeDtypeStruct(half, jnp.float32)),
        in_specs=[SMEM, VMEM, VMEM, VMEM],
        out_specs=(ANY, VMEM),
        compiler_params=SMALL,
        scratch_shapes=[pltpu.VMEM(half, jnp.float32), pltpu.SemaphoreType.DMA],
    )(place, own, far(ahead), far(behind))


def routed_kernel(
    place_ref, own_ref, got_ref, block_ref, kept_ref, sent_ref, held_ref, mine_ref, sems
):
    noff, tall, wide = held_ref.shape
    for k in range(noff):
        for c in range(wide // LANES):
            side, at = c * ROW // SUB, k * SUB + c * ROW % SUB
            tile = got_ref[:, side, at : at + ROW, :]
            held_ref[k, :, c * LANES : (c + 1) * LANES] = tile.reshape(tall, LANES)
    out = pltpu.make_async_copy(held_ref, block_ref, sems.at[0])
    out.start()
    pair_products(
        place_ref, own_ref, lambda k: held_ref[k], mine_ref, kept_ref, sent_ref, sems.at[1]
    ).wait()
    out.wait()


def partials_routed(place, own, got):
    tall, wide = own.shape
    noff = got.shape[1] // SUB
    got = got.reshape(tall // ROW, -1, noff * SUB, LANES)
    half, whole = (noff, tall // 2, tall), (noff, tall, wide)
    return pl.pallas_call(
        routed_kernel,
        out_shape=(
            pltpu.HBM(whole, own.dtype),
            pltpu.HBM(half, jnp.float32),
            jax.ShapeDtypeStruct(half, jnp.float32),
        ),
        in_specs=[SMEM, VMEM, VMEM],
        out_specs=(ANY, ANY, VMEM),
        compiler_params=SMALL,
        scratch_shapes=[
            pltpu.VMEM(whole, own.dtype),
            pltpu.VMEM(half, jnp.float32),
            pltpu.SemaphoreType.DMA((2,)),
        ],
    )(place, own, near(got))


def amplitude(place_ref, shift, occ_ref, row_ref, pair, there, amp_ref):
    me, core = place_ref[0], place_ref[1]
    half, _ = pair.shape
    energy = occ_ref[me] + occ_ref[lax.rem(me + shift, occ_ref.shape[0])]
    row = row_ref[...]
    for value, place in ((pair, core), (there, 1 - core)):
        start = pl.multiple_of(place * half, half)
        mine = row_ref[:, pl.ds(start, half)]
        column = jnp.broadcast_to(mine, (LANES, half)).T[:, :1]
        amp_ref[pl.ds(start, half), :] = value / (energy - column - row)
    return amp_ref[...]


def density_of(place_ref, amp_ref, mixed, rows):
    section = 2 * place_ref[2] + place_ref[1]
    at = pl.ds(pl.multiple_of(section * rows, rows), rows)
    return inner(amp_ref[at, :].astype(mixed.dtype), mixed)


def early_kernel(
    place_ref, shifts_ref, occ_ref, row_ref, pair_ref, there_ref, ahead_ref, behind_ref,
    gamma_ref, density_ref, amp_ref,
):
    rows = density_ref.shape[0]
    refs = (ahead_ref, behind_ref)
    for k in range(2):
        amp = amplitude(
            place_ref, shifts_ref[k], occ_ref, row_ref, pair_ref[k], there_ref[k], amp_ref
        )
        mixed = (2.0 * amp - amp.T).astype(ahead_ref.dtype)
        part = jnp.dot(mixed, refs[k][...], preferred_element_type=jnp.float32)
        gamma_ref[...] = part if k == 0 else gamma_ref[...] + part

        @pl.when(place_ref[3] == k)
        def _():
            density_ref[...] = density_of(place_ref, amp_ref, mixed, rows)


def early_pairs(place, shifts, occ, row, pair, there, ahead, behind):
    nvir, wide = ahead.shape
    return pl.pallas_call(
        early_kernel,
        out_shape=(
            pltpu.HBM((nvir, wide), jnp.float32),
            pltpu.HBM((nvir // 4, nvir), jnp.float32),
        ),
        in_specs=[SMEM, SMEM, SMEM, VMEM, VMEM, VMEM, VMEM, VMEM],
        out_specs=(VMEM, VMEM),
        compiler_params=SMALL,
        scratch_shapes=[pltpu.VMEM((nvir, nvir), jnp.float32)],
    )(place, shifts, occ, row, pair, there, far(ahead), far(behind))


def first_kernel(
    place_ref, shifts_ref, occ_ref, row_ref, pair_ref, there_ref, sofar_ref,
    mixed_ref, density_ref, amp_ref, held_ref, sem,
):
    amp = amplitude(
        place_ref, shifts_ref[2], occ_ref, row_ref, pair_ref[...], there_ref[...], amp_ref
    )
    held_ref[...] = (2.0 * amp - amp.T).astype(held_ref.dtype)
    out = pltpu.make_async_copy(held_ref, mixed_ref, sem)
    out.start()
    part = density_of(place_ref, amp_ref, held_ref[...], density_ref.shape[0])
    density_ref[...] = (sofar_ref[...] + part).astype(density_ref.dtype)
    out.wait()


def first_pair(place, shifts, occ, row, pair, there, sofar):
    _, nvir = pair.shape
    return pl.pallas_call(
        first_kernel,
        out_shape=(
            pltpu.HBM((nvir, nvir), jnp.bfloat16),
            pltpu.HBM(sofar.shape, jnp.bfloat16),
        ),
        in_specs=[SMEM, SMEM, SMEM, VMEM, VMEM, VMEM, VMEM],
        out_specs=(ANY, VMEM),
        compiler_params=SMALL,
        scratch_shapes=[
            pltpu.VMEM((nvir, nvir), jnp.float32),
            pltpu.VMEM((nvir, nvir), jnp.bfloat16),
            pltpu.SemaphoreType.DMA,
        ],
    )(place, shifts, occ, row, near(pair), near(there), sofar)


def rest_kernel(
    place_ref, shifts_ref, occ_ref, row_ref, pair_ref, there_ref, mixed_ref, blocks_ref,
    sofar_ref, gamma_ref, amp_ref, first_ref, block_ref, total_ref, sems,
):
    copies = [
        pltpu.make_async_copy(mixed_ref, first_ref, sems.at[0]),
        pltpu.make_async_copy(blocks_ref, block_ref, sems.at[1]),
        pltpu.make_async_copy(sofar_ref, total_ref, sems.at[2]),
    ]
    for copy in copies:
        copy.start()
    amp = amplitude(
        place_ref, shifts_ref[3], occ_ref, row_ref, pair_ref[...], there_ref[...], amp_ref
    )
    mixed = (2.0 * amp - amp.T).astype(block_ref.dtype)
    for copy in copies:
        copy.wait()
    part = jnp.dot(first_ref[...], block_ref[0], preferred_element_type=jnp.float32)
    part += jnp.dot(mixed, block_ref[1], preferred_element_type=jnp.float32)
    gamma_ref[...] = total_ref[...] + part


def add_rest(place, shifts, occ, row, pair, there, mixed, blocks, sofar):
    return pl.pallas_call(
        rest_kernel,
        out_shape=jax.ShapeDtypeStruct(sofar.shape, jnp.float32),
        in_specs=[SMEM, SMEM, SMEM, VMEM, VMEM, VMEM, ANY, ANY, ANY],
        out_specs=VMEM,
        compiler_params=SMALL,
        scratch_shapes=[
            pltpu.VMEM((pair.shape[1],) * 2, jnp.float32),
            pltpu.VMEM(mixed.shape, mixed.dtype),
            pltpu.VMEM(blocks.shape, blocks.dtype),
            pltpu.VMEM(sofar.shape, jnp.float32),
            pltpu.SemaphoreType.DMA((3,)),
        ],
    )(place, shifts, occ, row, pair, there, far(mixed), far(blocks), far(sofar))


def local(factors, offsets, occ_energy, vir_energy):
    sizes = [lax.axis_size(a) for a in OCC]
    count = lax.axis_size(OCC)
    chip = lax.axis_index("zl").astype(jnp.int32)
    core = lax.axis_index("core").astype(jnp.int32)
    own = factors[0]
    nvir = own.shape[0]
    rows = nvir // 4
    row = vir_energy[None, :]
    costs = [0] + [busiest_link(s, sizes) for s in range(1, count)]
    cost = jnp.array(costs, jnp.int32)[offsets]
    late = cost[1] < cost[0]
    direct = jnp.where(late, offsets[1], offsets[0])
    routed = jnp.where(late, offsets[0], offsets[1])
    step = jnp.minimum(direct, count - direct)
    flip = (direct != step).astype(jnp.int32)
    place = jnp.stack([lax.axis_index(OCC).astype(jnp.int32), core, chip, flip])
    shifts = jnp.stack([step, count - step, routed, count - routed])

    held = exchange(to_pieces(own), OCC)
    ahead, behind = fetch_both_ways(own, step, count)
    outgoing = rolled(shifts[2:], held)
    got = exchange(outgoing, OCC)

    kept, sent = partials_direct(place, own, ahead, behind)
    came = swap(sent, "core")
    total = kept + came
    sent = total.astype(jnp.bfloat16)
    came = swap(sent, "zl")
    pair = total + came.astype(jnp.float32)
    there = swap(pair, "core")
    gamma, density = early_pairs(
        place, shifts, occ_energy, row, pair, there, ahead, behind
    )

    blocks, kept, sent = partials_routed(place, own, got)
    came = swap(sent, "core")
    total = kept + came
    sent = total.astype(jnp.bfloat16)
    came = swap(sent[0], "zl")
    second = swap(sent[1], "zl")
    pair = total[0] + came.astype(jnp.float32)
    there = swap(pair, "core")
    mixed, density = first_pair(place, shifts, occ_energy, row, pair, there, density)
    chip_sum, second, _ = lax.optimization_barrier((total[1], second, density))
    pair = chip_sum + second.astype(jnp.float32)
    there = swap(pair, "core")
    gamma = add_rest(place, shifts, occ_energy, row, pair, there, mixed, blocks, gamma)

    ny = lax.axis_size("y")
    nrow = lax.axis_size(ROWS)
    came = exchange(density.reshape(ny, rows // ny, nvir), "y")
    summed = jnp.sum(came.astype(jnp.float32), axis=0).astype(jnp.bfloat16)
    sent = jnp.broadcast_to(summed, (nrow, *summed.shape))
    came = exchange(sent, ROWS)
    summed = jnp.sum(came.astype(jnp.float32), axis=0).astype(jnp.bfloat16)
    sent = jnp.broadcast_to(summed, (ny, *summed.shape))
    came = exchange(sent, "y")
    return (gamma[None], came.reshape(rows, nvir).astype(jnp.float32))


def solution(mesh):
    split = Mesh(
        mesh.devices.reshape(4, 4, 8, 2, 2), ("zh", "x", "y", "zl", "core")
    )
    aux = ("zl", "core")

    return jax.shard_map(
        local,
        mesh=split,
        in_specs=(P(OCC, None, aux), P(), P(), P()),
        out_specs=(P(OCC, None, aux), P(aux, None)),
        check_vma=False,
    )
```

```python
import functools

import jax
import jax.numpy as jnp
from jax import lax
from jax.experimental import pallas as pl
from jax.experimental.pallas import tpu as pltpu
from jax.sharding import Mesh
from jax.sharding import PartitionSpec as P

OCC = ("zh", "x", "y")
REST = ("zh", "x", "zl")
ROW = 8
SUB = 16
LANES = 128
VMEM = pl.BlockSpec(memory_space=pltpu.VMEM)
SMEM = pl.BlockSpec(memory_space=pltpu.SMEM)
ANY = pl.BlockSpec(memory_space=pl.ANY)
SMALL = pltpu.CompilerParams(vmem_limit_bytes=16 << 20)


def near(value):
    return pltpu.with_memory_space_constraint(value, pltpu.VMEM)


def far(value):
    return pltpu.with_memory_space_constraint(value, pltpu.HBM)


def exchange(value, axis):
    return lax.all_to_all(value, axis, split_axis=0, concat_axis=0, tiled=True)


def swap(value, axis):
    return lax.ppermute(value, axis, [(0, 1), (1, 0)])


def inner(left, right):
    return lax.dot_general(
        left, right, (((1,), (1,)), ((), ())), preferred_element_type=jnp.float32
    )


def to_pieces(block):
    tall, wide = block.shape
    tiles = block.reshape(tall // ROW, ROW, wide // LANES, LANES)
    return tiles.transpose(0, 2, 1, 3).reshape(-1, SUB, LANES)


def roll_kernel(starts_ref, held_ref, out_ref, twice_ref, sems):
    count = held_ref.shape[0]
    twice_ref[:count] = held_ref[...]
    twice_ref[count:] = held_ref[...]
    copies = []
    for k in range(starts_ref.shape[0]):
        copies.append(
            pltpu.make_async_copy(
                twice_ref.at[pl.ds(starts_ref[k], count)],
                out_ref.at[:, pl.ds(k * SUB, SUB), :],
                sems.at[k],
            )
        )
        copies[-1].start()
    for copy in copies:
        copy.wait()


def rolled(starts, held):
    count, sub, lanes = held.shape
    total = starts.shape[0]
    return pl.pallas_call(
        roll_kernel,
        out_shape=pltpu.HBM((count, total * sub, lanes), held.dtype),
        in_specs=[SMEM, VMEM],
        out_specs=ANY,
        compiler_params=SMALL,
        scratch_shapes=[
            pltpu.VMEM((2 * count, sub, lanes), held.dtype),
            pltpu.SemaphoreType.DMA((total,)),
        ],
    )(starts, near(held))


def partial_kernel(
    chip_first, place_ref, own_ref, got_ref, block_ref, kept_ref, sent_ref, held_ref, sem
):
    noff, tall, wide = held_ref.shape
    half = tall // 2
    core, chip = place_ref[1], place_ref[2]
    for k in range(noff):
        for c in range(wide // LANES):
            side, at = c * ROW // SUB, k * SUB + c * ROW % SUB
            tile = got_ref[:, side, at : at + ROW, :]
            held_ref[k, :, c * LANES : (c + 1) * LANES] = tile.reshape(tall, LANES)
    out = pltpu.make_async_copy(held_ref, block_ref, sem)
    out.start()
    mine = own_ref[pl.ds(pl.multiple_of(core * half, half), half), :]
    other = own_ref[pl.ds(pl.multiple_of((1 - core) * half, half), half), :]
    for k in range(noff):
        block = held_ref[(chip if k == 0 else 1 - chip) if chip_first else k]
        kept_ref[k] = inner(mine, block)
        sent_ref[k] = inner(other, block)
    out.wait()


def partials(place, own, got, chip_first):
    tall, wide = own.shape
    noff = got.shape[1] // SUB
    got = got.reshape(tall // ROW, -1, noff * SUB, LANES)
    half, whole = (noff, tall // 2, tall), (noff, tall, wide)
    return pl.pallas_call(
        functools.partial(partial_kernel, chip_first),
        out_shape=(
            pltpu.HBM(whole, own.dtype),
            pltpu.VMEM(half, jnp.float32),
            pltpu.VMEM(half, jnp.float32),
        ),
        in_specs=[SMEM, VMEM, VMEM],
        out_specs=(ANY, VMEM, VMEM),
        compiler_params=SMALL,
        scratch_shapes=[pltpu.VMEM(whole, own.dtype), pltpu.SemaphoreType.DMA],
    )(place, own, near(got))


def amplitude(place_ref, shift, occ_ref, row_ref, pair, there, amp_ref):
    me, core = place_ref[0], place_ref[1]
    half, _ = pair.shape
    energy = occ_ref[me] + occ_ref[lax.rem(me + shift, occ_ref.shape[0])]
    row = row_ref[...]
    for value, place in ((pair, core), (there, 1 - core)):
        start = pl.multiple_of(place * half, half)
        mine = row_ref[:, pl.ds(start, half)]
        column = jnp.broadcast_to(mine, (LANES, half)).T[:, :1]
        amp_ref[pl.ds(start, half), :] = value / (energy - column - row)
    return amp_ref[...]


def first_kernel(
    place_ref, shifts_ref, occ_ref, row_ref, pair_ref, there_ref,
    mixed_ref, density_ref, amp_ref, held_ref, sem,
):
    core, chip = place_ref[1], place_ref[2]
    slots, chips, depth, _ = density_ref.shape
    rows = slots * depth
    amp = amplitude(
        place_ref, shifts_ref[chip], occ_ref, row_ref, pair_ref[...], there_ref[...], amp_ref
    )
    held_ref[...] = (2.0 * amp - amp.T).astype(held_ref.dtype)
    out = pltpu.make_async_copy(held_ref, mixed_ref, sem)
    out.start()
    for s in range(chips):
        at = pl.ds(pl.multiple_of((chips * s + core) * rows, rows), rows)
        part = inner(amp_ref[at, :].astype(held_ref.dtype), held_ref[...])
        part = part.astype(density_ref.dtype)
        density_ref[:, s] = part.reshape(slots, depth, part.shape[1])
    out.wait()


def first_pair(place, shifts, occ, row, pair, there, slots):
    _, nvir = pair.shape
    return pl.pallas_call(
        first_kernel,
        out_shape=(
            pltpu.HBM((nvir, nvir), jnp.bfloat16),
            pltpu.HBM((slots, 2, nvir // 4 // slots, nvir), jnp.bfloat16),
        ),
        in_specs=[SMEM, SMEM, SMEM, VMEM, VMEM, VMEM],
        out_specs=(ANY, VMEM),
        compiler_params=SMALL,
        scratch_shapes=[
            pltpu.VMEM((nvir, nvir), jnp.float32),
            pltpu.VMEM((nvir, nvir), jnp.bfloat16),
            pltpu.SemaphoreType.DMA,
        ],
    )(place, shifts, occ, row, near(pair), near(there))


def product_kernel(place_ref, mixed_ref, block_ref, out_ref):
    block = block_ref[place_ref[2]]
    out_ref[...] = jnp.dot(mixed_ref[...], block, preferred_element_type=jnp.float32)


def product(place, mixed, block):
    return pl.pallas_call(
        product_kernel,
        out_shape=pltpu.HBM(block.shape[1:], jnp.float32),
        in_specs=[SMEM, VMEM, VMEM],
        out_specs=VMEM,
        compiler_params=SMALL,
    )(place, far(mixed), far(block))


def rest_kernel(
    place_ref, shifts_ref, occ_ref, row_ref, pair_ref, there_ref, ahead_ref, behind_ref,
    sofar_ref, gamma_ref, amp_ref, block_ref, total_ref, sems,
):
    other = 1 - place_ref[2]
    copies = [
        pltpu.make_async_copy(sofar_ref, total_ref, sems.at[0]),
        pltpu.make_async_copy(ahead_ref.at[other], block_ref.at[0], sems.at[1]),
        pltpu.make_async_copy(behind_ref, block_ref.at[pl.ds(1, 2)], sems.at[2]),
    ]
    for copy in copies:
        copy.start()
    for k in range(pair_ref.shape[0]):
        shift = shifts_ref[other if k == 0 else k + 1]
        amp = amplitude(place_ref, shift, occ_ref, row_ref, pair_ref[k], there_ref[k], amp_ref)
        mixed = (2.0 * amp - amp.T).astype(block_ref.dtype)
        if k == 0:
            copies[0].wait()
            copies[1].wait()
        if k == 1:
            copies[2].wait()
        part = jnp.dot(mixed, block_ref[k], preferred_element_type=jnp.float32)
        gamma_ref[...] = (total_ref[...] if k == 0 else gamma_ref[...]) + part


def add_rest(place, shifts, occ, row, pair, there, ahead, behind, sofar):
    npair = pair.shape[0]
    return pl.pallas_call(
        rest_kernel,
        out_shape=jax.ShapeDtypeStruct(sofar.shape, jnp.float32),
        in_specs=[SMEM, SMEM, SMEM, VMEM, VMEM, VMEM, ANY, ANY, ANY],
        out_specs=VMEM,
        compiler_params=SMALL,
        scratch_shapes=[
            pltpu.VMEM((pair.shape[2],) * 2, jnp.float32),
            pltpu.VMEM((npair, *ahead.shape[1:]), ahead.dtype),
            pltpu.VMEM(sofar.shape, jnp.float32),
            pltpu.SemaphoreType.DMA((3,)),
        ],
    )(place, shifts, occ, row, pair, there, far(ahead), far(behind), far(sofar))


def local(factors, offsets, occ_energy, vir_energy):
    count = lax.axis_size(OCC)
    chip = lax.axis_index("zl").astype(jnp.int32)
    core = lax.axis_index("core").astype(jnp.int32)
    place = jnp.stack([lax.axis_index(OCC).astype(jnp.int32), core, chip])
    own = factors[0]
    nvir = own.shape[0]
    rows = nvir // 4
    row = vir_energy[None, :]
    shifts = jnp.concatenate([offsets, count - offsets])

    held = exchange(to_pieces(own), OCC)
    outgoing = rolled(shifts[:2], held)
    got_ahead = exchange(outgoing, OCC)
    outgoing = rolled(shifts[2:], held)
    got_behind = exchange(outgoing, OCC)

    ahead, kept, sent = partials(place, own, got_ahead, True)
    came = swap(sent, "core")
    total = kept + came
    sent = total.astype(jnp.bfloat16)
    came = swap(sent[1], "zl")
    second = swap(sent[0], "zl")
    pair = total[0] + came.astype(jnp.float32)
    there = swap(pair, "core")
    mixed, density = first_pair(
        place, shifts, occ_energy, row, pair, there, lax.axis_size("y")
    )

    behind, kept, sent = partials(place, own, got_behind, False)
    came = swap(sent, "core")
    back = kept + came
    sent = back.astype(jnp.bfloat16)
    came = swap(sent, "zl")
    waiting, second, _ = lax.optimization_barrier((total[1], second, density))
    pair = jnp.concatenate([waiting[None], back]) + jnp.concatenate(
        [second[None], came]
    ).astype(jnp.float32)
    there = swap(pair, "core")
    sofar = product(place, mixed, ahead)
    gamma = add_rest(place, shifts, occ_energy, row, pair, there, ahead, behind, sofar)

    ny = lax.axis_size("y")
    nrest = lax.axis_size(REST) // 2
    came = exchange(density, "y")
    summed = jnp.sum(came.astype(jnp.float32), axis=0).astype(jnp.bfloat16)
    sent = jnp.broadcast_to(summed, (nrest, *summed.shape)).reshape(
        2 * nrest, rows // ny, nvir
    )
    came = exchange(sent, REST)
    summed = jnp.sum(came.astype(jnp.float32), axis=0).astype(jnp.bfloat16)
    sent = jnp.broadcast_to(summed, (ny, *summed.shape))
    came = exchange(sent, "y")
    return (gamma[None], came.reshape(rows, nvir).astype(jnp.float32))


def solution(mesh):
    split = Mesh(
        mesh.devices.reshape(4, 4, 8, 2, 2), ("zh", "x", "y", "zl", "core")
    )
    aux = ("zl", "core")

    return jax.shard_map(
        local,
        mesh=split,
        in_specs=(P(OCC, None, aux), P(), P(), P()),
        out_specs=(P(OCC, None, aux), P(aux, None)),
        check_vma=False,
    )
```

```python
import functools

import jax
import jax.numpy as jnp
from jax import lax
from jax.experimental import pallas as pl
from jax.experimental.pallas import tpu as pltpu
from jax.sharding import Mesh
from jax.sharding import PartitionSpec as P

OCC = ("zh", "x", "y")
ROW = 8
SUB = 16
LANES = 128
VMEM = pl.BlockSpec(memory_space=pltpu.VMEM)
SMEM = pl.BlockSpec(memory_space=pltpu.SMEM)
ANY = pl.BlockSpec(memory_space=pl.ANY)
SMALL = pltpu.CompilerParams(vmem_limit_bytes=16 << 20)


def near(value):
    return pltpu.with_memory_space_constraint(value, pltpu.VMEM)


def far(value):
    return pltpu.with_memory_space_constraint(value, pltpu.HBM)


def exchange(value, axis):
    return lax.all_to_all(value, axis, split_axis=0, concat_axis=0, tiled=True)


def swap(value, axis):
    return lax.ppermute(value, axis, [(0, 1), (1, 0)])


def inner(left, right):
    return lax.dot_general(
        left, right, (((1,), (1,)), ((), ())), preferred_element_type=jnp.float32
    )


def to_pieces(block):
    tall, wide = block.shape
    tiles = block.reshape(tall // ROW, ROW, wide // LANES, LANES)
    return tiles.transpose(0, 2, 1, 3).reshape(-1, SUB, LANES)


def roll_kernel(starts_ref, held_ref, out_ref, twice_ref, sems):
    count = held_ref.shape[0]
    twice_ref[:count] = held_ref[...]
    twice_ref[count:] = held_ref[...]
    copies = []
    for k in range(starts_ref.shape[0]):
        copies.append(
            pltpu.make_async_copy(
                twice_ref.at[pl.ds(starts_ref[k], count)],
                out_ref.at[:, pl.ds(k * SUB, SUB), :],
                sems.at[k],
            )
        )
        copies[-1].start()
    for copy in copies:
        copy.wait()


def rolled(starts, held):
    count, sub, lanes = held.shape
    total = starts.shape[0]
    return pl.pallas_call(
        roll_kernel,
        out_shape=pltpu.HBM((count, total * sub, lanes), held.dtype),
        in_specs=[SMEM, VMEM],
        out_specs=ANY,
        compiler_params=SMALL,
        scratch_shapes=[
            pltpu.VMEM((2 * count, sub, lanes), held.dtype),
            pltpu.SemaphoreType.DMA((total,)),
        ],
    )(starts, near(held))


def partial_kernel(
    group, place_ref, own_ref, got_ref, block_ref, kept_ref, sent_ref, held_ref, sem
):
    noff, tall, wide = held_ref.shape
    half = tall // 2
    core = place_ref[1]
    for k in range(noff):
        for c in range(wide // LANES):
            side, at = c * ROW // SUB, (group * noff + k) * SUB + c * ROW % SUB
            tile = got_ref[:, side, at : at + ROW, :]
            held_ref[k, :, c * LANES : (c + 1) * LANES] = tile.reshape(tall, LANES)
    out = pltpu.make_async_copy(held_ref, block_ref, sem)
    out.start()
    mine = own_ref[pl.ds(pl.multiple_of(core * half, half), half), :]
    other = own_ref[pl.ds(pl.multiple_of((1 - core) * half, half), half), :]
    for k in range(noff):
        sent_ref[k] = inner(other, held_ref[k])
        kept_ref[k] = inner(mine, held_ref[k])
    out.wait()


def partials(group, place, own, got):
    tall, wide = own.shape
    noff = got.shape[1] // SUB // 2
    got = got.reshape(tall // ROW, -1, 2 * noff * SUB, LANES)
    half, whole = (noff, tall // 2, tall), (noff, tall, wide)
    return pl.pallas_call(
        functools.partial(partial_kernel, group),
        out_shape=(
            pltpu.HBM(whole, own.dtype),
            jax.ShapeDtypeStruct(half, jnp.float32),
            jax.ShapeDtypeStruct(half, jnp.float32),
        ),
        in_specs=[SMEM, VMEM, VMEM],
        out_specs=(ANY, VMEM, VMEM),
        compiler_params=SMALL,
        scratch_shapes=[pltpu.VMEM(whole, own.dtype), pltpu.SemaphoreType.DMA],
    )(place, own, got)


def amplitude(place_ref, shift, occ_ref, row_ref, pair, there, amp_ref):
    me, core = place_ref[0], place_ref[1]
    half, _ = pair.shape
    energy = occ_ref[me] + occ_ref[lax.rem(me + shift, occ_ref.shape[0])]
    row = row_ref[...]
    for value, place in ((pair, core), (there, 1 - core)):
        start = pl.multiple_of(place * half, half)
        mine = row_ref[:, pl.ds(start, half)]
        column = jnp.broadcast_to(mine, (LANES, half)).T[:, :1]
        amp_ref[pl.ds(start, half), :] = value / (energy - column - row)
    return amp_ref[...]


def ahead_kernel(
    place_ref, shifts_ref, occ_ref, row_ref, pair_ref, there_ref,
    mixed_ref, density_ref, amp_ref, held_ref, sem,
):
    rows = density_ref.shape[0]
    section = 2 * place_ref[2] + place_ref[1]
    at = pl.ds(pl.multiple_of(section * rows, rows), rows)
    total = None
    for k in range(held_ref.shape[0]):
        amp = amplitude(
            place_ref, shifts_ref[k], occ_ref, row_ref, pair_ref[k], there_ref[k], amp_ref
        )
        held_ref[k] = (2.0 * amp - amp.T).astype(held_ref.dtype)
        part = inner(amp_ref[at, :].astype(held_ref.dtype), held_ref[k])
        total = part if total is None else total + part
    out = pltpu.make_async_copy(held_ref, mixed_ref, sem)
    out.start()
    density_ref[...] = total.astype(density_ref.dtype)
    out.wait()


def ahead_pairs(place, shifts, occ, row, pair, there):
    noff, _, nvir = pair.shape
    whole = (noff, nvir, nvir)
    return pl.pallas_call(
        ahead_kernel,
        out_shape=(
            pltpu.HBM(whole, jnp.bfloat16),
            jax.ShapeDtypeStruct((nvir // 4, nvir), jnp.bfloat16),
        ),
        in_specs=[SMEM, SMEM, SMEM, VMEM, VMEM, VMEM],
        out_specs=(ANY, VMEM),
        compiler_params=SMALL,
        scratch_shapes=[
            pltpu.VMEM((nvir, nvir), jnp.float32),
            pltpu.VMEM(whole, jnp.bfloat16),
            pltpu.SemaphoreType.DMA,
        ],
    )(place, shifts, occ, row, near(pair), near(there))


def product_kernel(mixed_ref, block_ref, out_ref):
    total = None
    for k in range(mixed_ref.shape[0]):
        part = jnp.dot(mixed_ref[k], block_ref[k], preferred_element_type=jnp.float32)
        total = part if total is None else total + part
    out_ref[...] = total


def product(mixed, block):
    return pl.pallas_call(
        product_kernel,
        out_shape=pltpu.HBM(block.shape[1:], jnp.float32),
        in_specs=[VMEM, VMEM],
        out_specs=VMEM,
        compiler_params=SMALL,
    )(far(mixed), far(block))


def rest_kernel(
    place_ref, shifts_ref, occ_ref, row_ref, pair_ref, there_ref, blocks_ref, sofar_ref,
    gamma_ref, amp_ref, block_ref, total_ref, sems,
):
    copies = [
        pltpu.make_async_copy(blocks_ref, block_ref, sems.at[0]),
        pltpu.make_async_copy(sofar_ref, total_ref, sems.at[1]),
    ]
    for copy in copies:
        copy.start()
    noff = pair_ref.shape[0]
    for k in range(noff):
        amp = amplitude(
            place_ref, shifts_ref[noff + k], occ_ref, row_ref, pair_ref[k], there_ref[k],
            amp_ref,
        )
        mixed = (2.0 * amp - amp.T).astype(block_ref.dtype)
        if k == 0:
            for copy in copies:
                copy.wait()
        part = jnp.dot(mixed, block_ref[k], preferred_element_type=jnp.float32)
        gamma_ref[...] = (total_ref[...] if k == 0 else gamma_ref[...]) + part


def add_rest(place, shifts, occ, row, pair, there, blocks, sofar):
    nvir = pair.shape[2]
    return pl.pallas_call(
        rest_kernel,
        out_shape=jax.ShapeDtypeStruct(sofar.shape, jnp.float32),
        in_specs=[SMEM, SMEM, SMEM, VMEM, VMEM, VMEM, ANY, ANY],
        out_specs=VMEM,
        compiler_params=SMALL,
        scratch_shapes=[
            pltpu.VMEM((nvir, nvir), jnp.float32),
            pltpu.VMEM(blocks.shape, blocks.dtype),
            pltpu.VMEM(sofar.shape, jnp.float32),
            pltpu.SemaphoreType.DMA((2,)),
        ],
    )(place, shifts, occ, row, pair, there, far(blocks), far(sofar))


def local(factors, offsets, occ_energy, vir_energy):
    count = lax.axis_size(OCC)
    chip = lax.axis_index("zl").astype(jnp.int32)
    core = lax.axis_index("core").astype(jnp.int32)
    place = jnp.stack([lax.axis_index(OCC).astype(jnp.int32), core, chip])
    own = factors[0]
    nvir = own.shape[0]
    rows = nvir // 4
    row = vir_energy[None, :]
    shifts = jnp.concatenate([offsets, count - offsets])

    held = exchange(to_pieces(own), OCC)
    outgoing = rolled(shifts, held)
    got = exchange(outgoing, OCC)

    ahead, kept, sent = partials(0, place, own, got)
    came = swap(sent, "core")
    total = kept + came
    sent = total.astype(jnp.bfloat16)
    came = swap(sent, "zl")
    pair = total + came.astype(jnp.float32)
    there = swap(pair, "core")
    mixed, density = ahead_pairs(place, shifts, occ_energy, row, pair, there)

    behind, kept, sent = partials(1, place, own, got)
    came = swap(sent, "core")
    back = kept + came
    sent = back.astype(jnp.bfloat16)
    came = swap(sent, "zl")
    back, came, _ = lax.optimization_barrier((back, came, density))
    pair = back + came.astype(jnp.float32)
    there = swap(pair, "core")
    sofar = product(mixed, ahead)
    gamma = add_rest(
        place, shifts, occ_energy, row, pair, there, behind, sofar
    )

    came = exchange(density.reshape(count, rows // count, nvir), OCC)
    summed = jnp.sum(came.astype(jnp.float32), axis=0).astype(jnp.bfloat16)
    sent = jnp.broadcast_to(summed, (count, *summed.shape))
    came = exchange(sent, OCC)
    return (gamma[None], came.reshape(rows, nvir).astype(jnp.float32))


def solution(mesh):
    split = Mesh(
        mesh.devices.reshape(4, 4, 8, 2, 2), ("zh", "x", "y", "zl", "core")
    )
    aux = ("zl", "core")

    return jax.shard_map(
        local,
        mesh=split,
        in_specs=(P(OCC, None, aux), P(), P(), P()),
        out_specs=(P(OCC, None, aux), P(aux, None)),
        check_vma=False,
    )
```

```python
import functools

import jax
import jax.numpy as jnp
from jax import lax
from jax.experimental import pallas as pl
from jax.experimental.pallas import tpu as pltpu
from jax.sharding import Mesh
from jax.sharding import PartitionSpec as P

OCC = ("zh", "x", "y")
ROW = 8
SUB = 16
LANES = 128
VMEM = pl.BlockSpec(memory_space=pltpu.VMEM)
SMEM = pl.BlockSpec(memory_space=pltpu.SMEM)
ANY = pl.BlockSpec(memory_space=pl.ANY)
SMALL = pltpu.CompilerParams(vmem_limit_bytes=16 << 20)


def near(value):
    return pltpu.with_memory_space_constraint(value, pltpu.VMEM)


def far(value):
    return pltpu.with_memory_space_constraint(value, pltpu.HBM)


def exchange(value, axis):
    return lax.all_to_all(value, axis, split_axis=0, concat_axis=0, tiled=True)


def swap(value, axis):
    return lax.ppermute(value, axis, [(0, 1), (1, 0)])


def inner(left, right):
    return lax.dot_general(
        left, right, (((1,), (1,)), ((), ())), preferred_element_type=jnp.float32
    )


def to_pieces(block):
    tall, wide = block.shape
    tiles = block.reshape(tall // ROW, ROW, wide // LANES, LANES)
    return tiles.transpose(0, 2, 1, 3).reshape(-1, SUB, LANES)


def roll_kernel(starts_ref, held_ref, out_ref, twice_ref, sems):
    count = held_ref.shape[0]
    twice_ref[:count] = held_ref[...]
    twice_ref[count:] = held_ref[...]
    copies = []
    for k in range(starts_ref.shape[0]):
        copies.append(
            pltpu.make_async_copy(
                twice_ref.at[pl.ds(starts_ref[k], count)],
                out_ref.at[:, pl.ds(k * SUB, SUB), :],
                sems.at[k],
            )
        )
        copies[-1].start()
    for copy in copies:
        copy.wait()


def rolled(starts, held):
    count, sub, lanes = held.shape
    total = starts.shape[0]
    return pl.pallas_call(
        roll_kernel,
        out_shape=pltpu.HBM((count, total * sub, lanes), held.dtype),
        in_specs=[SMEM, VMEM],
        out_specs=ANY,
        compiler_params=SMALL,
        scratch_shapes=[
            pltpu.VMEM((2 * count, sub, lanes), held.dtype),
            pltpu.SemaphoreType.DMA((total,)),
        ],
    )(starts, near(held))


def partial_kernel(
    group, place_ref, own_ref, got_ref, block_ref, kept_ref, sent_ref, held_ref, sem
):
    noff, tall, wide = held_ref.shape
    half = tall // 2
    core = place_ref[1]
    for k in range(noff):
        for c in range(wide // LANES):
            side, at = c * ROW // SUB, (group * noff + k) * SUB + c * ROW % SUB
            tile = got_ref[:, side, at : at + ROW, :]
            held_ref[k, :, c * LANES : (c + 1) * LANES] = tile.reshape(tall, LANES)
    out = pltpu.make_async_copy(held_ref, block_ref, sem)
    out.start()
    mine = own_ref[pl.ds(pl.multiple_of(core * half, half), half), :]
    other = own_ref[pl.ds(pl.multiple_of((1 - core) * half, half), half), :]
    for k in range(noff):
        sent_ref[k] = inner(other, held_ref[k])
        kept_ref[k] = inner(mine, held_ref[k])
    out.wait()


def partials(group, place, own, got):
    tall, wide = own.shape
    noff = got.shape[1] // SUB // 2
    got = got.reshape(tall // ROW, -1, 2 * noff * SUB, LANES)
    half, whole = (noff, tall // 2, tall), (noff, tall, wide)
    return pl.pallas_call(
        functools.partial(partial_kernel, group),
        out_shape=(
            pltpu.HBM(whole, own.dtype),
            jax.ShapeDtypeStruct(half, jnp.float32),
            jax.ShapeDtypeStruct(half, jnp.float32),
        ),
        in_specs=[SMEM, VMEM, VMEM],
        out_specs=(ANY, VMEM, VMEM),
        compiler_params=SMALL,
        scratch_shapes=[pltpu.VMEM(whole, own.dtype), pltpu.SemaphoreType.DMA],
    )(place, own, got)


def amplitude(place_ref, shift, occ_ref, row_ref, pair, there, amp_ref):
    me, core = place_ref[0], place_ref[1]
    half, _ = pair.shape
    energy = occ_ref[me] + occ_ref[lax.rem(me + shift, occ_ref.shape[0])]
    row = row_ref[...]
    for value, place in ((pair, core), (there, 1 - core)):
        start = pl.multiple_of(place * half, half)
        mine = row_ref[:, pl.ds(start, half)]
        column = jnp.broadcast_to(mine, (LANES, half)).T[:, :1]
        amp_ref[pl.ds(start, half), :] = value / (energy - column - row)
    return amp_ref[...]


def ahead_kernel(
    place_ref, shifts_ref, occ_ref, row_ref, pair_ref, there_ref,
    mixed_ref, density_ref, amp_ref, held_ref, sem,
):
    groups, cols, deep, lanes = density_ref.shape
    rows = groups * deep
    section = 2 * place_ref[2] + place_ref[1]
    at = pl.ds(pl.multiple_of(section * rows, rows), rows)
    total = None
    for k in range(held_ref.shape[0]):
        amp = amplitude(
            place_ref, shifts_ref[k], occ_ref, row_ref, pair_ref[k], there_ref[k], amp_ref
        )
        held_ref[k] = (2.0 * amp - amp.T).astype(held_ref.dtype)
        part = inner(amp_ref[at, :].astype(held_ref.dtype), held_ref[k])
        total = part if total is None else total + part
    out = pltpu.make_async_copy(held_ref, mixed_ref, sem)
    out.start()
    for c in range(cols):
        tile = total[:, c * lanes : (c + 1) * lanes].reshape(groups, deep, lanes)
        density_ref[:, c] = tile.astype(density_ref.dtype)
    out.wait()


def ahead_pairs(place, shifts, occ, row, pair, there):
    noff, _, nvir = pair.shape
    whole = (noff, nvir, nvir)
    return pl.pallas_call(
        ahead_kernel,
        out_shape=(
            pltpu.HBM(whole, jnp.bfloat16),
            jax.ShapeDtypeStruct((nvir // 16, nvir // LANES, 4, LANES), jnp.bfloat16),
        ),
        in_specs=[SMEM, SMEM, SMEM, VMEM, VMEM, VMEM],
        out_specs=(ANY, VMEM),
        compiler_params=SMALL,
        scratch_shapes=[
            pltpu.VMEM((nvir, nvir), jnp.float32),
            pltpu.VMEM(whole, jnp.bfloat16),
            pltpu.SemaphoreType.DMA,
        ],
    )(place, shifts, occ, row, near(pair), near(there))


def gamma_kernel(
    place_ref, shifts_ref, occ_ref, row_ref, pair_ref, there_ref, mixed_ref, ahead_ref,
    behind_ref, gamma_ref, amp_ref, first_ref, block_ref, sems,
):
    noff = pair_ref.shape[0]
    copies = [
        pltpu.make_async_copy(mixed_ref, first_ref, sems.at[0]),
        pltpu.make_async_copy(ahead_ref, block_ref.at[pl.ds(0, noff)], sems.at[1]),
        pltpu.make_async_copy(behind_ref, block_ref.at[pl.ds(noff, noff)], sems.at[2]),
    ]
    for copy in copies:
        copy.start()
    for k in range(noff):
        amp = amplitude(
            place_ref, shifts_ref[noff + k], occ_ref, row_ref, pair_ref[k], there_ref[k],
            amp_ref,
        )
        mixed = (2.0 * amp - amp.T).astype(block_ref.dtype)
        if k == 0:
            for copy in copies:
                copy.wait()
        part = jnp.dot(mixed, block_ref[noff + k], preferred_element_type=jnp.float32)
        part += jnp.dot(first_ref[k], block_ref[k], preferred_element_type=jnp.float32)
        gamma_ref[...] = part if k == 0 else gamma_ref[...] + part


def gamma_of(place, shifts, occ, row, pair, there, mixed, ahead, behind):
    noff, nvir, wide = ahead.shape
    return pl.pallas_call(
        gamma_kernel,
        out_shape=jax.ShapeDtypeStruct((nvir, wide), jnp.float32),
        in_specs=[SMEM, SMEM, SMEM, VMEM, VMEM, VMEM, ANY, ANY, ANY],
        out_specs=VMEM,
        compiler_params=SMALL,
        scratch_shapes=[
            pltpu.VMEM((nvir, nvir), jnp.float32),
            pltpu.VMEM(mixed.shape, mixed.dtype),
            pltpu.VMEM((2 * noff, nvir, wide), ahead.dtype),
            pltpu.SemaphoreType.DMA((3,)),
        ],
    )(place, shifts, occ, row, pair, there, far(mixed), far(ahead), far(behind))


def lines_kernel(tiles_ref, out_ref):
    groups, cols, deep, lanes = tiles_ref.shape
    for c in range(cols):
        tile = tiles_ref[:, c].astype(out_ref.dtype)
        out_ref[:, c * lanes : (c + 1) * lanes] = tile.reshape(groups * deep, lanes)


def to_lines(tiles):
    groups, cols, deep, lanes = tiles.shape
    return pl.pallas_call(
        lines_kernel,
        out_shape=jax.ShapeDtypeStruct((groups * deep, cols * lanes), jnp.float32),
        in_specs=[VMEM],
        out_specs=VMEM,
        compiler_params=SMALL,
    )(near(tiles))


def local(factors, offsets, occ_energy, vir_energy):
    count = lax.axis_size(OCC)
    chip = lax.axis_index("zl").astype(jnp.int32)
    core = lax.axis_index("core").astype(jnp.int32)
    place = jnp.stack([lax.axis_index(OCC).astype(jnp.int32), core, chip])
    own = factors[0]
    row = vir_energy[None, :]
    shifts = jnp.concatenate([offsets, count - offsets])

    held = exchange(to_pieces(own), OCC)
    outgoing = rolled(shifts, held)
    got = exchange(outgoing, OCC)

    ahead, kept, sent = partials(0, place, own, got)
    came = swap(sent, "core")
    total = kept + came
    sent = total.astype(jnp.bfloat16)
    came = swap(sent, "zl")
    pair = total + came.astype(jnp.float32)
    there = swap(pair, "core")
    mixed, density = ahead_pairs(place, shifts, occ_energy, row, pair, there)

    behind, kept, sent = partials(1, place, own, got)
    came = swap(sent, "core")
    back = kept + came
    sent = back.astype(jnp.bfloat16)
    came = swap(sent, "zl")
    pair = back + came.astype(jnp.float32)
    there = swap(pair, "core")
    gamma = gamma_of(place, shifts, occ_energy, row, pair, there, mixed, ahead, behind)

    came = exchange(density.reshape(count, -1, LANES), OCC)
    summed = jnp.sum(came.astype(jnp.float32), axis=0).astype(jnp.bfloat16)
    sent = jnp.broadcast_to(summed, (count, *summed.shape))
    came = exchange(sent, OCC)
    return (gamma[None], to_lines(came.reshape(density.shape)))


def solution(mesh):
    split = Mesh(
        mesh.devices.reshape(4, 4, 8, 2, 2), ("zh", "x", "y", "zl", "core")
    )
    aux = ("zl", "core")

    return jax.shard_map(
        local,
        mesh=split,
        in_specs=(P(OCC, None, aux), P(), P(), P()),
        out_specs=(P(OCC, None, aux), P(aux, None)),
        check_vma=False,
    )
```

```python
import functools

import jax
import jax.numpy as jnp
from jax import lax
from jax.experimental import pallas as pl
from jax.experimental.pallas import tpu as pltpu
from jax.sharding import Mesh
from jax.sharding import PartitionSpec as P

OCC = ("zh", "x", "y")
ROW = 8
SUB = 16
LANES = 128
VMEM = pl.BlockSpec(memory_space=pltpu.VMEM)
SMEM = pl.BlockSpec(memory_space=pltpu.SMEM)
ANY = pl.BlockSpec(memory_space=pl.ANY)
SMALL = pltpu.CompilerParams(vmem_limit_bytes=16 << 20)


def near(value):
    return pltpu.with_memory_space_constraint(value, pltpu.VMEM)


def far(value):
    return pltpu.with_memory_space_constraint(value, pltpu.HBM)


def exchange(value, axis):
    return lax.all_to_all(value, axis, split_axis=0, concat_axis=0, tiled=True)


def swap(value, axis):
    return lax.ppermute(value, axis, [(0, 1), (1, 0)])


def inner(left, right):
    return lax.dot_general(
        left, right, (((1,), (1,)), ((), ())), preferred_element_type=jnp.float32
    )


def to_pieces(block):
    tall, wide = block.shape
    tiles = block.reshape(tall // ROW, ROW, wide // LANES, LANES)
    return tiles.transpose(0, 2, 1, 3).reshape(-1, SUB, LANES)


def roll_kernel(starts_ref, held_ref, out_ref, twice_ref, sems):
    count = held_ref.shape[0]
    twice_ref[:count] = held_ref[...]
    twice_ref[count:] = held_ref[...]
    copies = []
    for k in range(starts_ref.shape[0]):
        copies.append(
            pltpu.make_async_copy(
                twice_ref.at[pl.ds(starts_ref[k], count)],
                out_ref.at[:, pl.ds(k * SUB, SUB), :],
                sems.at[k],
            )
        )
        copies[-1].start()
    for copy in copies:
        copy.wait()


def rolled(starts, held):
    count, sub, lanes = held.shape
    total = starts.shape[0]
    return pl.pallas_call(
        roll_kernel,
        out_shape=pltpu.HBM((count, total * sub, lanes), held.dtype),
        in_specs=[SMEM, VMEM],
        out_specs=ANY,
        compiler_params=SMALL,
        scratch_shapes=[
            pltpu.VMEM((2 * count, sub, lanes), held.dtype),
            pltpu.SemaphoreType.DMA((total,)),
        ],
    )(starts, near(held))


def partial_kernel(
    group, place_ref, own_ref, got_ref, block_ref, kept_ref, sent_ref, held_ref, sem
):
    noff, tall, wide = held_ref.shape
    half = tall // 2
    core = place_ref[1]
    for k in range(noff):
        for c in range(wide // LANES):
            side, at = c * ROW // SUB, (group * noff + k) * SUB + c * ROW % SUB
            tile = got_ref[:, side, at : at + ROW, :]
            held_ref[k, :, c * LANES : (c + 1) * LANES] = tile.reshape(tall, LANES)
    out = pltpu.make_async_copy(held_ref, block_ref, sem)
    out.start()
    mine = own_ref[pl.ds(pl.multiple_of(core * half, half), half), :]
    other = own_ref[pl.ds(pl.multiple_of((1 - core) * half, half), half), :]
    for k in range(noff):
        sent_ref[k] = inner(other, held_ref[k])
        kept_ref[k] = inner(mine, held_ref[k])
    out.wait()


def partials(group, place, own, got):
    tall, wide = own.shape
    noff = got.shape[1] // SUB // 2
    got = got.reshape(tall // ROW, -1, 2 * noff * SUB, LANES)
    half, whole = (noff, tall // 2, tall), (noff, tall, wide)
    return pl.pallas_call(
        functools.partial(partial_kernel, group),
        out_shape=(
            pltpu.HBM(whole, own.dtype),
            jax.ShapeDtypeStruct(half, jnp.float32),
            jax.ShapeDtypeStruct(half, jnp.float32),
        ),
        in_specs=[SMEM, VMEM, VMEM],
        out_specs=(ANY, VMEM, VMEM),
        compiler_params=SMALL,
        scratch_shapes=[pltpu.VMEM(whole, own.dtype), pltpu.SemaphoreType.DMA],
    )(place, own, got)


def half_kernel(
    first, place_ref, shifts_ref, occ_ref, row_ref, total_ref, came_ref, amp_ref
):
    pairs, half, _ = amp_ref.shape
    me, core = place_ref[0], place_ref[1]
    row = row_ref[...]
    mine = row_ref[:, pl.ds(pl.multiple_of(core * half, half), half)]
    column = jnp.broadcast_to(mine, (LANES, half)).T[:, :1]
    for k in range(pairs):
        shift = shifts_ref[first + k]
        energy = occ_ref[me] + occ_ref[lax.rem(me + shift, occ_ref.shape[0])]
        at = (first + k) % total_ref.shape[0]
        pair = total_ref[at] + came_ref[k].astype(jnp.float32)
        amp_ref[k] = pair / (energy - column - row)


def half_amplitudes(first, place, shifts, occ, row, total, came):
    return pl.pallas_call(
        functools.partial(half_kernel, first),
        out_shape=jax.ShapeDtypeStruct(came.shape, jnp.float32),
        in_specs=[SMEM, SMEM, SMEM, VMEM, VMEM, VMEM],
        out_specs=VMEM,
        compiler_params=SMALL,
    )(place, shifts, occ, row, near(total), near(came))


def whole_of(place_ref, mine, there, amp_ref):
    half = mine.shape[0]
    core = place_ref[1]
    amp_ref[pl.ds(pl.multiple_of(core * half, half), half), :] = mine
    amp_ref[pl.ds(pl.multiple_of((1 - core) * half, half), half), :] = there
    return amp_ref[...]


def mixed_of(amp):
    return (2.0 * amp - amp.T).astype(jnp.bfloat16)


def density_of(place_ref, amp_ref, mixed, rows):
    section = 2 * place_ref[2] + place_ref[1]
    at = pl.ds(pl.multiple_of(section * rows, rows), rows)
    return inner(amp_ref[at, :].astype(mixed.dtype), mixed)


def first_kernel(
    place_ref, mine_ref, there_ref, mixed_ref, density_ref, amp_ref, held_ref, sem
):
    held_ref[...] = mixed_of(whole_of(place_ref, mine_ref[0], there_ref[0], amp_ref))
    out = pltpu.make_async_copy(held_ref, mixed_ref, sem)
    out.start()
    density_ref[...] = density_of(
        place_ref, amp_ref, held_ref[...], density_ref.shape[0]
    )
    out.wait()


def second_kernel(
    place_ref, mine_ref, there_ref, sofar_ref, mixed_ref, density_ref, amp_ref, held_ref,
    sem,
):
    groups, cols, deep, lanes = density_ref.shape
    held_ref[...] = mixed_of(whole_of(place_ref, mine_ref[0], there_ref[0], amp_ref))
    out = pltpu.make_async_copy(held_ref, mixed_ref, sem)
    out.start()
    total = sofar_ref[...] + density_of(
        place_ref, amp_ref, held_ref[...], sofar_ref.shape[0]
    )
    for c in range(cols):
        tile = total[:, c * lanes : (c + 1) * lanes].reshape(groups, deep, lanes)
        density_ref[:, c] = tile.astype(density_ref.dtype)
    out.wait()


def mix(place, mine, there, *sofar):
    nvir = mine.shape[2]
    lines = jax.ShapeDtypeStruct((nvir // 4, nvir), jnp.float32)
    tiles = jax.ShapeDtypeStruct((nvir // 16, nvir // LANES, 4, LANES), jnp.bfloat16)
    return pl.pallas_call(
        second_kernel if sofar else first_kernel,
        out_shape=(
            pltpu.HBM((nvir, nvir), jnp.bfloat16),
            tiles if sofar else lines,
        ),
        in_specs=[SMEM] + [VMEM] * (2 + len(sofar)),
        out_specs=(ANY, VMEM),
        compiler_params=SMALL,
        scratch_shapes=[
            pltpu.VMEM((nvir, nvir), jnp.float32),
            pltpu.VMEM((nvir, nvir), jnp.bfloat16),
            pltpu.SemaphoreType.DMA,
        ],
    )(place, near(mine), near(there), *sofar)


def gamma_kernel(
    place_ref, mine_ref, there_ref, first_ref, second_ref, ahead_ref, behind_ref, gamma_ref,
    amp_ref, held_ref, block_ref, sems,
):
    noff = mine_ref.shape[0]
    copies = [
        pltpu.make_async_copy(first_ref, held_ref.at[0], sems.at[0]),
        pltpu.make_async_copy(second_ref, held_ref.at[1], sems.at[1]),
        pltpu.make_async_copy(ahead_ref, block_ref.at[pl.ds(0, noff)], sems.at[2]),
        pltpu.make_async_copy(behind_ref, block_ref.at[pl.ds(noff, noff)], sems.at[3]),
    ]
    for copy in copies:
        copy.start()
    for k in range(noff):
        mixed = mixed_of(whole_of(place_ref, mine_ref[k], there_ref[k], amp_ref))
        if k == 0:
            for copy in copies:
                copy.wait()
        part = jnp.dot(mixed, block_ref[noff + k], preferred_element_type=jnp.float32)
        part += jnp.dot(held_ref[k], block_ref[k], preferred_element_type=jnp.float32)
        gamma_ref[...] = part if k == 0 else gamma_ref[...] + part


def gamma_of(place, mine, there, first, second, ahead, behind):
    noff, nvir, wide = ahead.shape
    return pl.pallas_call(
        gamma_kernel,
        out_shape=jax.ShapeDtypeStruct((nvir, wide), jnp.float32),
        in_specs=[SMEM, VMEM, VMEM, ANY, ANY, ANY, ANY],
        out_specs=VMEM,
        compiler_params=SMALL,
        scratch_shapes=[
            pltpu.VMEM((nvir, nvir), jnp.float32),
            pltpu.VMEM((noff, nvir, nvir), first.dtype),
            pltpu.VMEM((2 * noff, nvir, wide), ahead.dtype),
            pltpu.SemaphoreType.DMA((4,)),
        ],
    )(place, mine, there, far(first), far(second), far(ahead), far(behind))


def lines_kernel(tiles_ref, out_ref):
    groups, cols, deep, lanes = tiles_ref.shape
    for c in range(cols):
        tile = tiles_ref[:, c].astype(out_ref.dtype)
        out_ref[:, c * lanes : (c + 1) * lanes] = tile.reshape(groups * deep, lanes)


def to_lines(tiles):
    groups, cols, deep, lanes = tiles.shape
    return pl.pallas_call(
        lines_kernel,
        out_shape=jax.ShapeDtypeStruct((groups * deep, cols * lanes), jnp.float32),
        in_specs=[VMEM],
        out_specs=VMEM,
        compiler_params=SMALL,
    )(near(tiles))


def local(factors, offsets, occ_energy, vir_energy):
    count = lax.axis_size(OCC)
    chip = lax.axis_index("zl").astype(jnp.int32)
    core = lax.axis_index("core").astype(jnp.int32)
    place = jnp.stack([lax.axis_index(OCC).astype(jnp.int32), core, chip])
    own = factors[0]
    row = vir_energy[None, :]
    shifts = jnp.concatenate([offsets, count - offsets])

    held = exchange(to_pieces(own), OCC)
    outgoing = rolled(shifts, held)
    got = exchange(outgoing, OCC)

    ahead, kept, sent = partials(0, place, own, got)
    came = swap(sent, "core")
    total = kept + came
    sent = total.astype(jnp.bfloat16)
    came = swap(sent[:1], "zl")
    later = swap(sent[1:], "zl")
    amp = half_amplitudes(0, place, shifts, occ_energy, row, total, came)
    there = swap(amp, "core")
    first, density = mix(place, amp, there)
    amp = half_amplitudes(1, place, shifts, occ_energy, row, total, later)
    there = swap(amp, "core")
    second, density = mix(place, amp, there, density)

    behind, kept, sent = partials(1, place, own, got)
    came = swap(sent, "core")
    back = kept + came
    sent = back.astype(jnp.bfloat16)
    came = swap(sent, "zl")
    amp = half_amplitudes(2, place, shifts, occ_energy, row, back, came)
    there = swap(amp, "core")
    gamma = gamma_of(place, amp, there, first, second, ahead, behind)

    came = exchange(density.reshape(count, -1, LANES), OCC)
    summed = jnp.sum(came.astype(jnp.float32), axis=0).astype(jnp.bfloat16)
    sent = jnp.broadcast_to(summed, (count, *summed.shape))
    came = exchange(sent, OCC)
    return (gamma[None], to_lines(came.reshape(density.shape)))


def solution(mesh):
    split = Mesh(
        mesh.devices.reshape(4, 4, 8, 2, 2), ("zh", "x", "y", "zl", "core")
    )
    aux = ("zl", "core")

    return jax.shard_map(
        local,
        mesh=split,
        in_specs=(P(OCC, None, aux), P(), P(), P()),
        out_specs=(P(OCC, None, aux), P(aux, None)),
        check_vma=False,
    )
```

```python
import functools

import jax
import jax.numpy as jnp
from jax import lax
from jax.experimental import pallas as pl
from jax.experimental.pallas import tpu as pltpu
from jax.sharding import Mesh
from jax.sharding import PartitionSpec as P

OCC = ("zh", "x", "y")
PLANE = ("x", "y")
ROW = 8
SUB = 16
LANES = 128
VMEM = pl.BlockSpec(memory_space=pltpu.VMEM)
SMEM = pl.BlockSpec(memory_space=pltpu.SMEM)
ANY = pl.BlockSpec(memory_space=pl.ANY)
SMALL = pltpu.CompilerParams(vmem_limit_bytes=16 << 20)


def near(value):
    return pltpu.with_memory_space_constraint(value, pltpu.VMEM)


def far(value):
    return pltpu.with_memory_space_constraint(value, pltpu.HBM)


def exchange(value, axis):
    return lax.all_to_all(value, axis, split_axis=0, concat_axis=0, tiled=True)


def swap(value, axis):
    return lax.ppermute(value, axis, [(0, 1), (1, 0)])


def inner(left, right):
    return lax.dot_general(
        left, right, (((1,), (1,)), ((), ())), preferred_element_type=jnp.float32
    )


def to_pieces(block):
    tall, wide = block.shape
    tiles = block.reshape(tall // ROW, ROW, wide // LANES, LANES)
    return tiles.transpose(0, 2, 1, 3).reshape(-1, SUB, LANES)


def roll_kernel(starts_ref, held_ref, out_ref, twice_ref, sems):
    count = held_ref.shape[0]
    twice_ref[:count] = held_ref[...]
    twice_ref[count:] = held_ref[...]
    copies = []
    for k in range(starts_ref.shape[0]):
        copies.append(
            pltpu.make_async_copy(
                twice_ref.at[pl.ds(starts_ref[k], count)],
                out_ref.at[:, pl.ds(k * SUB, SUB), :],
                sems.at[k],
            )
        )
        copies[-1].start()
    for copy in copies:
        copy.wait()


def rolled(starts, held):
    count, sub, lanes = held.shape
    total = starts.shape[0]
    return pl.pallas_call(
        roll_kernel,
        out_shape=pltpu.HBM((count, total * sub, lanes), held.dtype),
        in_specs=[SMEM, VMEM],
        out_specs=ANY,
        compiler_params=SMALL,
        scratch_shapes=[
            pltpu.VMEM((2 * count, sub, lanes), held.dtype),
            pltpu.SemaphoreType.DMA((total,)),
        ],
    )(starts, near(held))


def partial_kernel(
    group, place_ref, own_ref, got_ref, block_ref, kept_ref, sent_ref, held_ref, sem
):
    noff, tall, wide = held_ref.shape
    half = tall // 2
    core = place_ref[1]
    for k in range(noff):
        for c in range(wide // LANES):
            side, at = c * ROW // SUB, (group * noff + k) * SUB + c * ROW % SUB
            tile = got_ref[:, side, at : at + ROW, :]
            held_ref[k, :, c * LANES : (c + 1) * LANES] = tile.reshape(tall, LANES)
    out = pltpu.make_async_copy(held_ref, block_ref, sem)
    out.start()
    mine = own_ref[pl.ds(pl.multiple_of(core * half, half), half), :]
    other = own_ref[pl.ds(pl.multiple_of((1 - core) * half, half), half), :]
    for k in range(noff):
        sent_ref[k] = inner(other, held_ref[k])
        kept_ref[k] = inner(mine, held_ref[k])
    out.wait()


def partials(group, place, own, got):
    tall, wide = own.shape
    noff = got.shape[1] // SUB // 2
    got = got.reshape(tall // ROW, -1, 2 * noff * SUB, LANES)
    half, whole = (noff, tall // 2, tall), (noff, tall, wide)
    return pl.pallas_call(
        functools.partial(partial_kernel, group),
        out_shape=(
            pltpu.HBM(whole, own.dtype),
            jax.ShapeDtypeStruct(half, jnp.float32),
            jax.ShapeDtypeStruct(half, jnp.float32),
        ),
        in_specs=[SMEM, VMEM, VMEM],
        out_specs=(ANY, VMEM, VMEM),
        compiler_params=SMALL,
        scratch_shapes=[pltpu.VMEM(whole, own.dtype), pltpu.SemaphoreType.DMA],
    )(place, own, got)


def amplitude(place_ref, shift, occ_ref, row_ref, pair, there, amp_ref):
    me, core = place_ref[0], place_ref[1]
    half, _ = pair.shape
    energy = occ_ref[me] + occ_ref[lax.rem(me + shift, occ_ref.shape[0])]
    row = row_ref[...]
    for value, place in ((pair, core), (there, 1 - core)):
        start = pl.multiple_of(place * half, half)
        mine = row_ref[:, pl.ds(start, half)]
        column = jnp.broadcast_to(mine, (LANES, half)).T[:, :1]
        amp_ref[pl.ds(start, half), :] = value / (energy - column - row)
    return amp_ref[...]


def ahead_kernel(
    place_ref, shifts_ref, occ_ref, row_ref, pair_ref, there_ref,
    mixed_ref, density_ref, amp_ref, held_ref, sem,
):
    groups, cols, deep, lanes = density_ref.shape
    rows = groups * deep
    section = 2 * place_ref[2] + place_ref[1]
    at = pl.ds(pl.multiple_of(section * rows, rows), rows)
    total = None
    for k in range(held_ref.shape[0]):
        amp = amplitude(
            place_ref, shifts_ref[k], occ_ref, row_ref, pair_ref[k], there_ref[k], amp_ref
        )
        held_ref[k] = (2.0 * amp - amp.T).astype(held_ref.dtype)
        part = inner(amp_ref[at, :].astype(held_ref.dtype), held_ref[k])
        total = part if total is None else total + part
    out = pltpu.make_async_copy(held_ref, mixed_ref, sem)
    out.start()
    for c in range(cols):
        tile = total[:, c * lanes : (c + 1) * lanes].reshape(groups, deep, lanes)
        density_ref[:, c] = tile.astype(density_ref.dtype)
    out.wait()


def ahead_pairs(place, shifts, occ, row, pair, there):
    noff, _, nvir = pair.shape
    whole = (noff, nvir, nvir)
    return pl.pallas_call(
        ahead_kernel,
        out_shape=(
            pltpu.HBM(whole, jnp.bfloat16),
            jax.ShapeDtypeStruct((nvir // 16, nvir // LANES, 4, LANES), jnp.bfloat16),
        ),
        in_specs=[SMEM, SMEM, SMEM, VMEM, VMEM, VMEM],
        out_specs=(ANY, VMEM),
        compiler_params=SMALL,
        scratch_shapes=[
            pltpu.VMEM((nvir, nvir), jnp.float32),
            pltpu.VMEM(whole, jnp.bfloat16),
            pltpu.SemaphoreType.DMA,
        ],
    )(place, shifts, occ, row, near(pair), near(there))


def gamma_kernel(
    place_ref, shifts_ref, occ_ref, row_ref, pair_ref, there_ref, mixed_ref, ahead_ref,
    behind_ref, gamma_ref, amp_ref, first_ref, block_ref, sems,
):
    noff = pair_ref.shape[0]
    copies = [
        pltpu.make_async_copy(mixed_ref, first_ref, sems.at[0]),
        pltpu.make_async_copy(ahead_ref, block_ref.at[pl.ds(0, noff)], sems.at[1]),
        pltpu.make_async_copy(behind_ref, block_ref.at[pl.ds(noff, noff)], sems.at[2]),
    ]
    for copy in copies:
        copy.start()
    for k in range(noff):
        amp = amplitude(
            place_ref, shifts_ref[noff + k], occ_ref, row_ref, pair_ref[k], there_ref[k],
            amp_ref,
        )
        mixed = (2.0 * amp - amp.T).astype(block_ref.dtype)
        if k == 0:
            for copy in copies:
                copy.wait()
        part = jnp.dot(mixed, block_ref[noff + k], preferred_element_type=jnp.float32)
        part += jnp.dot(first_ref[k], block_ref[k], preferred_element_type=jnp.float32)
        gamma_ref[...] = part if k == 0 else gamma_ref[...] + part


def gamma_of(place, shifts, occ, row, pair, there, mixed, ahead, behind):
    noff, nvir, wide = ahead.shape
    return pl.pallas_call(
        gamma_kernel,
        out_shape=jax.ShapeDtypeStruct((nvir, wide), jnp.float32),
        in_specs=[SMEM, SMEM, SMEM, VMEM, VMEM, VMEM, ANY, ANY, ANY],
        out_specs=VMEM,
        compiler_params=SMALL,
        scratch_shapes=[
            pltpu.VMEM((nvir, nvir), jnp.float32),
            pltpu.VMEM(mixed.shape, mixed.dtype),
            pltpu.VMEM((2 * noff, nvir, wide), ahead.dtype),
            pltpu.SemaphoreType.DMA((3,)),
        ],
    )(place, shifts, occ, row, pair, there, far(mixed), far(ahead), far(behind))


def lines_kernel(tiles_ref, out_ref):
    parts, groups, cols, deep, lanes = tiles_ref.shape
    for c in range(cols):
        total = tiles_ref[0, :, c].astype(out_ref.dtype)
        for p in range(1, parts):
            total += tiles_ref[p, :, c].astype(out_ref.dtype)
        out_ref[:, c * lanes : (c + 1) * lanes] = total.reshape(groups * deep, lanes)


def to_lines(tiles):
    _, groups, cols, deep, lanes = tiles.shape
    return pl.pallas_call(
        lines_kernel,
        out_shape=jax.ShapeDtypeStruct((groups * deep, cols * lanes), jnp.float32),
        in_specs=[VMEM],
        out_specs=VMEM,
        compiler_params=SMALL,
    )(near(tiles))


def local(factors, offsets, occ_energy, vir_energy):
    count = lax.axis_size(OCC)
    chip = lax.axis_index("zl").astype(jnp.int32)
    core = lax.axis_index("core").astype(jnp.int32)
    place = jnp.stack([lax.axis_index(OCC).astype(jnp.int32), core, chip])
    own = factors[0]
    row = vir_energy[None, :]
    shifts = jnp.concatenate([offsets, count - offsets])

    held = exchange(to_pieces(own), OCC)
    outgoing = rolled(shifts, held)
    got = exchange(outgoing, OCC)

    ahead, kept, sent = partials(0, place, own, got)
    came = swap(sent, "core")
    total = kept + came
    sent = total.astype(jnp.bfloat16)
    came = swap(sent, "zl")
    pair = total + came.astype(jnp.float32)
    there = swap(pair, "core")
    mixed, density = ahead_pairs(place, shifts, occ_energy, row, pair, there)

    behind, kept, sent = partials(1, place, own, got)
    came = swap(sent, "core")
    back = kept + came
    sent = back.astype(jnp.bfloat16)
    came = swap(sent, "zl")
    pair = back + came.astype(jnp.float32)
    there = swap(pair, "core")
    gamma = gamma_of(place, shifts, occ_energy, row, pair, there, mixed, ahead, behind)

    came = exchange(density, PLANE)
    summed = jnp.sum(came.astype(jnp.float32), axis=0).astype(jnp.bfloat16)
    sent = jnp.broadcast_to(summed, (count, *summed.shape))
    came = exchange(sent, OCC)
    return (gamma[None], to_lines(came.reshape(-1, *density.shape)))


def solution(mesh):
    split = Mesh(
        mesh.devices.reshape(4, 4, 8, 2, 2), ("zh", "x", "y", "zl", "core")
    )
    aux = ("zl", "core")

    return jax.shard_map(
        local,
        mesh=split,
        in_specs=(P(OCC, None, aux), P(), P(), P()),
        out_specs=(P(OCC, None, aux), P(aux, None)),
        check_vma=False,
    )
```
